512 devices in a mesh: groups: 2 (over y), row: 128 (over z, x), col: 2 (over core).
Axes of the slice: x: 4, y: 2, z: 32, core: 2. Of those that a mesh axis runs over, the one named last changes fastest.
The devices are a block of a 4x8x32 slice.
Arguments:
- pair_act: bfloat16 [1024, 512, 128], P(('groups', 'row'), 'col'), parts along dimension 0, may hold values from -6 to 6
- in_gain: float32 [128], replicated, may hold values from 0.5 to 1.5
- in_shift: float32 [128], replicated, may hold values from -1 to 1
- left_weight: bfloat16 [128, 256], replicated, may hold values from -0.5 to 0.5
- left_bias: float32 [256], replicated, may hold values from -3 to 3
- right_weight: bfloat16 [128, 256], replicated, may hold values from -0.5 to 0.5
- right_bias: float32 [256], replicated, may hold values from -3 to 3
- gate_weight: bfloat16 [128, 128], replicated, may hold values from -0.5 to 0.5
- gate_bias: float32 [128], replicated, may hold values from -4 to 4
- out_gain: float32 [128], replicated, may hold values from 0.8 to 1.2
- out_shift: float32 [128], replicated, may hold values from -3 to 3
- out_weight: bfloat16 [128, 128], replicated, may hold values from -1 to 1
- out_bias: float32 [128], replicated, may hold values from -3 to 3
Outputs:
- update: bfloat16 [1024, 512, 128], P(('groups', 'row'), 'col'), parts along dimension 0
The draws below stay inside these ranges and needn't reach their ends.
There are 2 independent parts, one for each index of `groups`. The reference program is written for one: setup_inputs(seed, part) draws one part's arguments, and reference() takes and returns one part's arrays. A program takes and returns all parts, laid end to end along the dimension named above; an argument that names none is the same for every part. Nothing has to cross between parts.
All inputs are finite; a program needn't handle non-finite values.
Results may differ from the reference program's by a relative error of at most 0.0061.
Values may be sent and summed in bfloat16 or wider, within the bound.
No kernel may reach another device: no remote copies, remote signals or barrier semaphores. Data moves between devices by JAX's collectives and lax.ppermute only.
A program may use at most 64 MiB of HBM per device.

```python
import jax
import jax.numpy as jnp
from jax import lax

CZ = 128
CH = 128
N = 512


def bias_halves(base_key):
    gate_key, value_key = jax.random.split(base_key)
    gate_part = jnp.clip(0.7 * jax.random.normal(gate_key, (CH,), jnp.float32), -3.0, 3.0)
    value_part = jnp.clip(0.15 * jax.random.normal(value_key, (CH,), jnp.float32), -0.3, 0.3)
    return jnp.concatenate([gate_part, value_part], axis=0)


def draw_left_bias(key, part):
    return bias_halves(jax.random.fold_in(key, 11))


def draw_right_bias(key, part):
    return bias_halves(jax.random.fold_in(key, 12))


def draw_out_weight(key, part):
    inner_key = jax.random.fold_in(key, 13)
    raw_rows = jnp.clip(jax.random.normal(inner_key, (CH, CZ), jnp.float32), -4.0, 4.0)
    row_norms = jnp.sqrt(jnp.sum(raw_rows * raw_rows, axis=1, keepdims=True) + 1e-06)
    scaled = raw_rows / row_norms
    return scaled.astype(jnp.bfloat16)


def level_of(stream_key, shape, pieces, low, top_value):
    level, own = 1.0, jax.random.fold_in(stream_key, 6)
    for axis_at, shards_of in pieces:
        steps = jnp.exp(jax.random.uniform(jax.random.fold_in(own, axis_at), (shards_of,), jnp.float32, low / len(pieces), top_value / len(pieces)))
        level = level * jnp.repeat(steps, shape[axis_at] // shards_of).reshape([-1 if axis == axis_at else 1 for axis in range(len(shape))])
    return level


def centred(stream_key, shape, deviation, reach, cuts=(), held_as=jnp.bfloat16):
    array = jax.random.normal(stream_key, shape, jnp.float32) * deviation
    if len(cuts) > 0:
        array = level_of(stream_key, shape, cuts, -0.22, 0.18) * array
    return jnp.clip(array, min=-reach, max=reach).astype(held_as)


def setup_inputs(seed: int = 0, part: int = 0) -> dict:
    seeds = jax.random.split(jax.random.key(seed), 14)
    own_keys = jax.random.split(jax.random.fold_in(seeds[13], part), 14)
    pair_act = centred(own_keys[0], (N, N, CZ), 1.0, 6.0, ((0, 128), (1, 2)))
    in_gain = jnp.clip(jax.random.uniform(seeds[1], (CZ,), jnp.float32, 0.5, 1.5), 0.5, 1.5)
    in_shift = centred(seeds[2], (CZ,), 0.2, 1.0, (), jnp.float32)
    left_weight = centred(seeds[3], (CZ, 2 * CH), CZ ** -0.5, 0.5)
    left_bias = draw_left_bias(jax.random.fold_in(seeds[13], 71), part)
    right_weight = centred(seeds[5], (CZ, 2 * CH), CZ ** -0.5, 0.5)
    right_bias = draw_right_bias(jax.random.fold_in(seeds[13], 71), part)
    gate_weight = centred(seeds[7], (CZ, CZ), CZ ** -0.5, 0.5)
    gate_bias = centred(seeds[8], (CZ,), 1.0, 4.0, (), jnp.float32)
    out_gain = jnp.clip(jax.random.uniform(seeds[9], (CH,), jnp.float32, 0.8, 1.2), 0.8, 1.2)
    out_shift = centred(seeds[10], (CH,), 0.5, 3.0, (), jnp.float32)
    out_weight = draw_out_weight(jax.random.fold_in(seeds[13], 71), part)
    out_bias = centred(seeds[12], (CZ,), 0.5, 3.0, (), jnp.float32)
    return dict(pair_act=pair_act, in_gain=in_gain, in_shift=in_shift, left_weight=left_weight, left_bias=left_bias, right_weight=right_weight, right_bias=right_bias, gate_weight=gate_weight, gate_bias=gate_bias, out_gain=out_gain, out_shift=out_shift, out_weight=out_weight, out_bias=out_bias)


def layer_norm(values, gain, shift, axis):
    center = values - lax.optimization_barrier(jnp.mean(values, axis=axis, keepdims=True))
    spread = lax.optimization_barrier(jnp.mean(center * center, axis=axis, keepdims=True))
    return center * lax.rsqrt(spread + 1e-05) * gain + shift

def edge_projection(flat, weight, bias, hidden):
    joined = jnp.dot(flat, weight, preferred_element_type=jnp.float32) + bias
    return (jax.nn.sigmoid(joined[:, :hidden]) * joined[:, hidden:]).astype(jnp.bfloat16)

def channel_product(operands):
    return jnp.dot(operands[0], operands[1].T, preferred_element_type=jnp.float32).astype(jnp.bfloat16)

def reference(pair_act, in_gain, in_shift, left_weight, left_bias, right_weight, right_bias, gate_weight, gate_bias, out_gain, out_shift, out_weight, out_bias):
    length = pair_act.shape[0]
    chans = pair_act.shape[2]
    hidden = left_weight.shape[1] // 2
    normed = layer_norm(pair_act.astype(jnp.float32), in_gain, in_shift, 2).astype(jnp.bfloat16)
    flat = normed.reshape(length * length, chans)
    left_edge = edge_projection(flat, left_weight, left_bias, hidden)
    right_edge = edge_projection(flat, right_weight, right_bias, hidden)
    gate = jax.nn.sigmoid(jnp.dot(flat, gate_weight, preferred_element_type=jnp.float32) + gate_bias)
    left_chan = left_edge.reshape(length, length, hidden).transpose(2, 0, 1)
    right_chan = right_edge.reshape(length, length, hidden).transpose(2, 0, 1)
    triangle = lax.map(channel_product, (left_chan, right_chan))
    triangle_flat = triangle.transpose(1, 2, 0).reshape(length * length, hidden)
    mixed = layer_norm(triangle_flat.astype(jnp.float32), out_gain, out_shift, 1).astype(jnp.bfloat16)
    projected = jnp.dot(mixed, out_weight, preferred_element_type=jnp.float32) + out_bias
    update = (gate * projected).astype(jnp.bfloat16)
    return update.reshape(length, length, chans)
```

```python
import jax
import jax.numpy as jnp
from jax import lax
from jax.experimental import pallas as pl
from jax.experimental.pallas import tpu as pltpu
from jax.sharding import PartitionSpec as P

LANES = 128


def column(row, width):
    return jnp.broadcast_to(row, (width, row.shape[1])).T


def edges_kernel(
    pair_ref, gain_ref, shift_ref, lw_ref, lb_ref, rw_ref, rb_ref, gw_ref, gb_ref,
    edge_ref, gate_ref, held_ref,
):
    rows, cols, chans = pair_ref.shape
    hidden = lw_ref.shape[1] // 2
    values = pair_ref[...].reshape(rows * cols, chans).astype(jnp.float32)
    center = values - jnp.mean(values, axis=1, keepdims=True)
    spread = jnp.mean(center * center, axis=1, keepdims=True)
    normed = (center * lax.rsqrt(spread + 1e-05) * gain_ref[...] + shift_ref[...]).astype(jnp.bfloat16)
    for side, (w_ref, b_ref) in enumerate(((lw_ref, lb_ref), (rw_ref, rb_ref))):
        gate_bias = column(b_ref[:, :hidden], LANES)[:, :1]
        value_bias = column(b_ref[:, hidden:], LANES)[:, :1]
        turned = w_ref[...].T
        for r in range(rows):
            part = normed[r * cols : (r + 1) * cols]
            joined = lax.dot_general(
                turned, part, (((1,), (1,)), ((), ())), preferred_element_type=jnp.float32
            )
            edge = jax.nn.sigmoid(joined[:hidden] + gate_bias) * (joined[hidden:] + value_bias)
            held_ref[:, r, side * cols : (side + 1) * cols] = edge
    edge_ref[...] = held_ref[...].astype(jnp.bfloat16)
    gate_ref[...] = jax.nn.sigmoid(
        jnp.dot(normed, gw_ref[...], preferred_element_type=jnp.float32) + gb_ref[...]
    )


def update_kernel(tri_ref, gate_ref, gain_ref, shift_ref, w_ref, b_ref, out_ref, held_ref):
    hidden, subs, lanes = tri_ref.shape
    values = tri_ref[...].astype(jnp.float32)
    center = values - jnp.mean(values, axis=0, keepdims=True)
    spread = jnp.mean(center * center, axis=0, keepdims=True)
    held_ref[...] = center * lax.rsqrt(spread + 1e-05)
    gain = column(gain_ref[...], lanes)
    shift = column(shift_ref[...], lanes)
    for s in range(subs):
        mixed = (held_ref[:, s, :] * gain + shift).astype(jnp.bfloat16)
        projected = lax.dot_general(
            mixed, w_ref[...], (((0,), (0,)), ((), ())), preferred_element_type=jnp.float32
        )
        at = slice(s * lanes, (s + 1) * lanes)
        out_ref[at, :] = (gate_ref[at, :] * (projected + b_ref[...])).astype(jnp.bfloat16)


def per_device(
    pair_act,
    in_gain,
    in_shift,
    left_weight,
    left_bias,
    right_weight,
    right_bias,
    gate_weight,
    gate_bias,
    out_gain,
    out_shift,
    out_weight,
    out_bias,
):
    rows, cols, chans = pair_act.shape
    hidden = left_weight.shape[1] // 2
    spots = rows * cols
    peers = lax.axis_size("row")
    halves = lax.axis_size("col")
    length = peers * rows

    def row(v):
        return v.reshape(1, -1)

    edges, gate = pl.pallas_call(
        edges_kernel,
        out_shape=(
            jax.ShapeDtypeStruct((hidden, rows, 2 * cols), jnp.bfloat16),
            jax.ShapeDtypeStruct((spots, chans), jnp.float32),
        ),
        scratch_shapes=[pltpu.VMEM((hidden, rows, 2 * cols), jnp.float32)],
    )(
        pair_act, row(in_gain), row(in_shift), left_weight, row(left_bias),
        right_weight, row(right_bias), gate_weight, row(gate_bias),
    )
    got = lax.all_to_all(edges, "row", split_axis=0, concat_axis=0, tiled=True)
    got = got.reshape(length, 2 * cols)
    left, right = got[:, :cols], got[:, cols:]
    me = lax.axis_index("col")
    half = length // halves

    def partial_sums(which):
        some = lax.dynamic_slice_in_dim(right, which * half, half, axis=0)
        return lax.dot_general(
            left, some, (((1,), (1,)), ((), ())), preferred_element_type=jnp.float32
        )

    away = lax.ppermute(partial_sums(1 - me), "col", [(0, 1), (1, 0)])
    triangle = (partial_sums(me) + away).astype(jnp.bfloat16)
    triangle = lax.all_to_all(
        triangle.reshape(peers, spots // LANES, LANES), "row", split_axis=0, concat_axis=0, tiled=True
    )
    update = pl.pallas_call(
        update_kernel,
        out_shape=jax.ShapeDtypeStruct((spots, chans), jnp.bfloat16),
        scratch_shapes=[pltpu.VMEM((hidden, spots // LANES, LANES), jnp.float32)],
    )(triangle, gate, row(out_gain), row(out_shift), out_weight, row(out_bias))
    return update.reshape(rows, cols, chans)


def solution(mesh):
    in_specs = (P(("groups", "row"), "col", None),) + (P(),) * 12
    out_specs = P(("groups", "row"), "col", None)
    return jax.shard_map(
        per_device, mesh=mesh, in_specs=in_specs, out_specs=out_specs, check_vma=False
    )
```

```python
import jax
import jax.numpy as jnp
from jax import lax
from jax.experimental import pallas as pl
from jax.experimental.pallas import tpu as pltpu
from jax.sharding import PartitionSpec as P

LANES = 128
SMALL = pltpu.CompilerParams(vmem_limit_bytes=16 * 2**20)


def column(row, width):
    return jnp.broadcast_to(row, (width, row.shape[1])).T


def edges_kernel(*refs):
    hbm, (edge_ref, gate_ref), held_ref, vmem, sems = refs[:9], refs[9:11], refs[11], refs[12:21], refs[21]
    loads = [pltpu.make_async_copy(h, v, sems.at[n]) for n, (h, v) in enumerate(zip(hbm, vmem))]
    for load in loads:
        load.start()
    pair_ref, gain_ref, shift_ref, lw_ref, lb_ref, rw_ref, rb_ref, gw_ref, gb_ref = vmem
    rows, cols, chans = pair_ref.shape
    hidden = lw_ref.shape[1] // 2
    for load in loads[:3]:
        load.wait()
    values = pair_ref[...].reshape(rows * cols, chans).astype(jnp.float32)
    center = values - jnp.mean(values, axis=1, keepdims=True)
    spread = jnp.mean(center * center, axis=1, keepdims=True)
    normed = (center * lax.rsqrt(spread + 1e-05) * gain_ref[...] + shift_ref[...]).astype(jnp.bfloat16)
    for load in loads[3:]:
        load.wait()
    for side, (w_ref, b_ref) in enumerate(((lw_ref, lb_ref), (rw_ref, rb_ref))):
        gate_bias = column(b_ref[:, :hidden], LANES)[:, :1]
        value_bias = column(b_ref[:, hidden:], LANES)[:, :1]
        turned = w_ref[...].T
        for r in range(rows):
            part = normed[r * cols : (r + 1) * cols]
            joined = lax.dot_general(
                turned, part, (((1,), (1,)), ((), ())), preferred_element_type=jnp.float32
            )
            edge = jax.nn.sigmoid(joined[:hidden] + gate_bias) * (joined[hidden:] + value_bias)
            held_ref[:, r, side * cols : (side + 1) * cols] = edge
    edge_ref[...] = held_ref[...].astype(jnp.bfloat16)
    gate_ref[...] = jax.nn.sigmoid(
        jnp.dot(normed, gw_ref[...], preferred_element_type=jnp.float32) + gb_ref[...]
    )


def update_kernel(tri_ref, gate_ref, gain_ref, shift_ref, w_ref, b_ref, out_ref, held_ref):
    hidden, subs, lanes = tri_ref.shape
    values = tri_ref[...].astype(jnp.float32)
    center = values - jnp.mean(values, axis=0, keepdims=True)
    spread = jnp.mean(center * center, axis=0, keepdims=True)
    held_ref[...] = center * lax.rsqrt(spread + 1e-05)
    gain = column(gain_ref[...], lanes)
    shift = column(shift_ref[...], lanes)
    for s in range(subs):
        mixed = (held_ref[:, s, :] * gain + shift).astype(jnp.bfloat16)
        projected = lax.dot_general(
            mixed, w_ref[...], (((0,), (0,)), ((), ())), preferred_element_type=jnp.float32
        )
        at = slice(s * lanes, (s + 1) * lanes)
        out_ref[at, :] = (gate_ref[at, :] * (projected + b_ref[...])).astype(jnp.bfloat16)


def per_device(
    pair_act,
    in_gain,
    in_shift,
    left_weight,
    left_bias,
    right_weight,
    right_bias,
    gate_weight,
    gate_bias,
    out_gain,
    out_shift,
    out_weight,
    out_bias,
):
    rows, cols, chans = pair_act.shape
    hidden = left_weight.shape[1] // 2
    spots = rows * cols
    peers = lax.axis_size("row")
    halves = lax.axis_size("col")
    length = peers * rows

    def row(v):
        return v.reshape(1, -1)

    given = (
        pair_act, row(in_gain), row(in_shift), left_weight, row(left_bias),
        right_weight, row(right_bias), gate_weight, row(gate_bias),
    )
    edges, gate = pl.pallas_call(
        edges_kernel,
        out_shape=(
            jax.ShapeDtypeStruct((hidden, rows, 2 * cols), jnp.bfloat16),
            jax.ShapeDtypeStruct((spots, chans), jnp.float32),
        ),
        in_specs=[pl.BlockSpec(memory_space=pltpu.HBM)] * len(given),
        scratch_shapes=[
            pltpu.VMEM((hidden, rows, 2 * cols), jnp.float32),
            *(pltpu.VMEM(v.shape, v.dtype) for v in given),
            pltpu.SemaphoreType.DMA((len(given),)),
        ],
        compiler_params=SMALL,
    )(*(pltpu.with_memory_space_constraint(v, pltpu.HBM) for v in given))
    half = length // halves
    me = lax.axis_index("col").astype(jnp.uint32)
    edges, mine, other = lax.optimization_barrier((edges, me * half, (1 - me) * half))
    got = lax.all_to_all(edges, "row", split_axis=0, concat_axis=0, tiled=True)
    got = got.reshape(length, 2 * cols)
    left, right = got[:, :cols], got[:, cols:]

    def partial_sums(start):
        some = lax.dynamic_slice_in_dim(right, start, half, axis=0)
        return lax.dot_general(
            left, some, (((1,), (1,)), ((), ())), preferred_element_type=jnp.float32
        )

    away = lax.ppermute(partial_sums(other), "col", [(0, 1), (1, 0)])
    triangle = (partial_sums(mine) + away).astype(jnp.bfloat16)
    triangle = lax.all_to_all(
        triangle.reshape(peers, spots // LANES, LANES), "row", split_axis=0, concat_axis=0, tiled=True
    )
    update = pl.pallas_call(
        update_kernel,
        out_shape=jax.ShapeDtypeStruct((spots, chans), jnp.bfloat16),
        scratch_shapes=[pltpu.VMEM((hidden, spots // LANES, LANES), jnp.float32)],
        compiler_params=SMALL,
    )(triangle, gate, row(out_gain), row(out_shift), out_weight, row(out_bias))
    return update.reshape(rows, cols, chans)


def solution(mesh):
    in_specs = (P(("groups", "row"), "col", None),) + (P(),) * 12
    out_specs = P(("groups", "row"), "col", None)
    return jax.shard_map(
        per_device, mesh=mesh, in_specs=in_specs, out_specs=out_specs, check_vma=False
    )
```

```python
import jax
import jax.numpy as jnp
from jax import lax
from jax.experimental import pallas as pl
from jax.experimental.pallas import tpu as pltpu
from jax.sharding import PartitionSpec as P

LANES = 128
SMALL = pltpu.CompilerParams(vmem_limit_bytes=16 * 2**20)


def column(row, width):
    return jnp.broadcast_to(row, (width, row.shape[1])).T


def edges_kernel(*refs):
    hbm, edge_ref, gate_ref, kept, held_ref = refs[:13], refs[13], refs[14], refs[15:19], refs[19]
    vmem, sems = refs[20:29], refs[29]
    loads = [pltpu.make_async_copy(h, v, sems.at[n]) for n, (h, v) in enumerate(zip(hbm, vmem + kept))]
    for load in loads:
        load.start()
    pair_ref, gain_ref, shift_ref, lw_ref, lb_ref, rw_ref, rb_ref, gw_ref, gb_ref = vmem
    rows, cols, chans = pair_ref.shape
    hidden = lw_ref.shape[1] // 2
    for load in loads[:3]:
        load.wait()
    values = pair_ref[...].reshape(rows * cols, chans).astype(jnp.float32)
    center = values - jnp.mean(values, axis=1, keepdims=True)
    spread = jnp.mean(center * center, axis=1, keepdims=True)
    normed = (center * lax.rsqrt(spread + 1e-05) * gain_ref[...] + shift_ref[...]).astype(jnp.bfloat16)
    for load in loads[3:]:
        load.wait()
    for side, (w_ref, b_ref) in enumerate(((lw_ref, lb_ref), (rw_ref, rb_ref))):
        gate_bias = column(b_ref[:, :hidden], LANES)[:, :1]
        value_bias = column(b_ref[:, hidden:], LANES)[:, :1]
        turned = w_ref[...].T
        for r in range(rows):
            part = normed[r * cols : (r + 1) * cols]
            joined = lax.dot_general(
                turned, part, (((1,), (1,)), ((), ())), preferred_element_type=jnp.float32
            )
            edge = jax.nn.sigmoid(joined[:hidden] + gate_bias) * (joined[hidden:] + value_bias)
            held_ref[:, r, side * cols : (side + 1) * cols] = edge
    edge_ref[...] = held_ref[...].astype(jnp.bfloat16)
    gate_ref[...] = jax.nn.sigmoid(
        jnp.dot(normed, gw_ref[...], preferred_element_type=jnp.float32) + gb_ref[...]
    )


def update_kernel(tri_ref, gate_ref, gain_ref, shift_ref, w_ref, b_ref, out_ref, held_ref):
    hidden, subs, lanes = tri_ref.shape
    values = tri_ref[...].astype(jnp.float32)
    center = values - jnp.mean(values, axis=0, keepdims=True)
    spread = jnp.mean(center * center, axis=0, keepdims=True)
    held_ref[...] = center * lax.rsqrt(spread + 1e-05)
    gain = column(gain_ref[...], lanes)
    shift = column(shift_ref[...], lanes)
    for s in range(subs):
        mixed = (held_ref[:, s, :] * gain + shift).astype(jnp.bfloat16)
        projected = lax.dot_general(
            mixed, w_ref[...], (((0,), (0,)), ((), ())), preferred_element_type=jnp.float32
        )
        at = slice(s * lanes, (s + 1) * lanes)
        out_ref[at, :] = (gate_ref[at, :] * (projected + b_ref[...])).astype(jnp.bfloat16)


def per_device(
    pair_act,
    in_gain,
    in_shift,
    left_weight,
    left_bias,
    right_weight,
    right_bias,
    gate_weight,
    gate_bias,
    out_gain,
    out_shift,
    out_weight,
    out_bias,
):
    rows, cols, chans = pair_act.shape
    hidden = left_weight.shape[1] // 2
    spots = rows * cols
    peers = lax.axis_size("row")
    halves = lax.axis_size("col")
    length = peers * rows

    def row(v):
        return v.reshape(1, -1)

    given = (
        pair_act, row(in_gain), row(in_shift), left_weight, row(left_bias),
        right_weight, row(right_bias), gate_weight, row(gate_bias),
    )
    closing = (row(out_gain), row(out_shift), out_weight, row(out_bias))
    edges, gate, *closing = pl.pallas_call(
        edges_kernel,
        out_shape=(
            jax.ShapeDtypeStruct((hidden, rows, 2 * cols), jnp.bfloat16),
            jax.ShapeDtypeStruct((spots, chans), jnp.float32),
            *(jax.ShapeDtypeStruct(v.shape, v.dtype) for v in closing),
        ),
        in_specs=[pl.BlockSpec(memory_space=pltpu.HBM)] * (len(given) + len(closing)),
        scratch_shapes=[
            pltpu.VMEM((hidden, rows, 2 * cols), jnp.float32),
            *(pltpu.VMEM(v.shape, v.dtype) for v in given),
            pltpu.SemaphoreType.DMA((len(given) + len(closing),)),
        ],
        compiler_params=SMALL,
    )(*(pltpu.with_memory_space_constraint(v, pltpu.HBM) for v in (*given, *closing)))
    half = length // halves
    me = lax.axis_index("col").astype(jnp.uint32)
    order = [(peers // 2 + n) % peers for n in range(peers)]
    edges, mine, other = lax.optimization_barrier((edges, (1 - me) * half, me * half))
    got = lax.all_to_all(edges, "row", split_axis=0, concat_axis=0, axis_index_groups=[order], tiled=True)
    got = got.reshape(length, 2 * cols)
    left, right = got[:, :cols], got[:, cols:]

    def partial_sums(start):
        some = lax.dynamic_slice_in_dim(right, start, half, axis=0)
        return lax.dot_general(
            left, some, (((1,), (1,)), ((), ())), preferred_element_type=jnp.float32
        )

    away = lax.ppermute(partial_sums(other), "col", [(0, 1), (1, 0)])
    triangle = (partial_sums(mine) + away).astype(jnp.bfloat16)
    triangle = lax.all_to_all(
        triangle.reshape(peers, spots // LANES, LANES), "row", split_axis=0, concat_axis=0, axis_index_groups=[order], tiled=True
    )
    update = pl.pallas_call(
        update_kernel,
        out_shape=jax.ShapeDtypeStruct((spots, chans), jnp.bfloat16),
        scratch_shapes=[pltpu.VMEM((hidden, spots // LANES, LANES), jnp.float32)],
        compiler_params=SMALL,
    )(triangle, gate, *closing)
    return update.reshape(rows, cols, chans)


def solution(mesh):
    in_specs = (P(("groups", "row"), "col", None),) + (P(),) * 12
    out_specs = P(("groups", "row"), "col", None)
    return jax.shard_map(
        per_device, mesh=mesh, in_specs=in_specs, out_specs=out_specs, check_vma=False
    )
```

```python
import jax
import jax.numpy as jnp
from jax import lax
from jax.experimental import pallas as pl
from jax.experimental.pallas import tpu as pltpu
from jax.sharding import PartitionSpec as P

LANES = 128
SMALL = pltpu.CompilerParams(vmem_limit_bytes=16 * 2**20)


def column(row, width):
    return jnp.broadcast_to(row, (width, row.shape[1])).T


def edges_kernel(*refs):
    hbm, edge_ref, gate_ref, kept, held_ref = refs[:13], refs[13], refs[14], refs[15:19], refs[19]
    vmem, sems = refs[20:29], refs[29]
    loads = [pltpu.make_async_copy(h, v, sems.at[n]) for n, (h, v) in enumerate(zip(hbm, vmem + kept))]
    for load in loads:
        load.start()
    pair_ref, gain_ref, shift_ref, lw_ref, lb_ref, rw_ref, rb_ref, gw_ref, gb_ref = vmem
    rows, cols, chans = pair_ref.shape
    hidden = lw_ref.shape[1] // 2
    for load in loads[:3]:
        load.wait()
    values = pair_ref[...].reshape(rows * cols, chans).astype(jnp.float32)
    center = values - jnp.mean(values, axis=1, keepdims=True)
    spread = jnp.mean(center * center, axis=1, keepdims=True)
    normed = (center * lax.rsqrt(spread + 1e-05) * gain_ref[...] + shift_ref[...]).astype(jnp.bfloat16)
    for load in loads[3:]:
        load.wait()
    for side, (w_ref, b_ref) in enumerate(((lw_ref, lb_ref), (rw_ref, rb_ref))):
        gate_bias = column(b_ref[:, :hidden], LANES)[:, :1]
        value_bias = column(b_ref[:, hidden:], LANES)[:, :1]
        turned = w_ref[...].T
        for r in range(rows):
            part = normed[r * cols : (r + 1) * cols]
            joined = lax.dot_general(
                turned, part, (((1,), (1,)), ((), ())), preferred_element_type=jnp.float32
            )
            edge = jax.nn.sigmoid(joined[:hidden] + gate_bias) * (joined[hidden:] + value_bias)
            at = slice(side * cols, (side + 1) * cols)
            held_ref[: hidden // 2, r, at] = edge[hidden // 2 :]
            held_ref[hidden // 2 :, r, at] = edge[: hidden // 2]
    edge_ref[...] = held_ref[...].astype(jnp.bfloat16)
    gate_ref[...] = jax.nn.sigmoid(
        jnp.dot(normed, gw_ref[...], preferred_element_type=jnp.float32) + gb_ref[...]
    )


def update_kernel(tri_ref, gate_ref, gain_ref, shift_ref, w_ref, b_ref, out_ref, held_ref):
    hidden, subs, lanes = tri_ref.shape
    values = tri_ref[...].astype(jnp.float32)
    center = values - jnp.mean(values, axis=0, keepdims=True)
    spread = jnp.mean(center * center, axis=0, keepdims=True)
    held_ref[...] = center * lax.rsqrt(spread + 1e-05)
    gain = column(gain_ref[...], lanes)
    shift = column(shift_ref[...], lanes)
    for s in range(subs):
        mixed = (held_ref[:, s, :] * gain + shift).astype(jnp.bfloat16)
        projected = lax.dot_general(
            mixed, w_ref[...], (((0,), (0,)), ((), ())), preferred_element_type=jnp.float32
        )
        at = slice(s * lanes, (s + 1) * lanes)
        out_ref[at, :] = (gate_ref[at, :] * (projected + b_ref[...])).astype(jnp.bfloat16)


def per_device(
    pair_act,
    in_gain,
    in_shift,
    left_weight,
    left_bias,
    right_weight,
    right_bias,
    gate_weight,
    gate_bias,
    out_gain,
    out_shift,
    out_weight,
    out_bias,
):
    rows, cols, chans = pair_act.shape
    hidden = left_weight.shape[1] // 2
    spots = rows * cols
    peers = lax.axis_size("row")
    halves = lax.axis_size("col")
    length = peers * rows

    def row(v):
        return v.reshape(1, -1)

    given = (
        pair_act, row(in_gain), row(in_shift), left_weight, row(left_bias),
        right_weight, row(right_bias), gate_weight, row(gate_bias),
    )
    closing = (row(out_gain), row(out_shift), out_weight, row(out_bias))
    edges, gate, *closing = pl.pallas_call(
        edges_kernel,
        out_shape=(
            jax.ShapeDtypeStruct((hidden, rows, 2 * cols), jnp.bfloat16),
            jax.ShapeDtypeStruct((spots, chans), jnp.float32),
            *(jax.ShapeDtypeStruct(v.shape, v.dtype) for v in closing),
        ),
        in_specs=[pl.BlockSpec(memory_space=pltpu.HBM)] * (len(given) + len(closing)),
        scratch_shapes=[
            pltpu.VMEM((hidden, rows, 2 * cols), jnp.float32),
            *(pltpu.VMEM(v.shape, v.dtype) for v in given),
            pltpu.SemaphoreType.DMA((len(given) + len(closing),)),
        ],
        compiler_params=SMALL,
    )(*(pltpu.with_memory_space_constraint(v, pltpu.HBM) for v in (*given, *closing)))
    half = length // halves
    me = lax.axis_index("col").astype(jnp.uint32)
    order = [(peers // 2 + n) % peers for n in range(peers)]
    edges, mine, other = lax.optimization_barrier((edges, me * half, (1 - me) * half))
    got = lax.all_to_all(edges, "row", split_axis=0, concat_axis=0, tiled=True)
    got = got.reshape(length, 2 * cols)
    middle = length // 2
    left = jnp.concatenate((got[middle:, :cols], got[:middle, :cols]))
    right = got[:, cols:]

    def partial_sums(start):
        some = lax.dynamic_slice_in_dim(right, start, half, axis=0)
        return lax.dot_general(
            left, some, (((1,), (1,)), ((), ())), preferred_element_type=jnp.float32
        )

    away = lax.ppermute(partial_sums(other), "col", [(0, 1), (1, 0)])
    triangle = (partial_sums(mine) + away).astype(jnp.bfloat16)
    triangle = lax.all_to_all(
        triangle.reshape(peers, spots // LANES, LANES), "row", split_axis=0, concat_axis=0, axis_index_groups=[order], tiled=True
    )
    update = pl.pallas_call(
        update_kernel,
        out_shape=jax.ShapeDtypeStruct((spots, chans), jnp.bfloat16),
        scratch_shapes=[pltpu.VMEM((hidden, spots // LANES, LANES), jnp.float32)],
        compiler_params=SMALL,
    )(triangle, gate, *closing)
    return update.reshape(rows, cols, chans)


def solution(mesh):
    in_specs = (P(("groups", "row"), "col", None),) + (P(),) * 12
    out_specs = P(("groups", "row"), "col", None)
    return jax.shard_map(
        per_device, mesh=mesh, in_specs=in_specs, out_specs=out_specs, check_vma=False
    )
```

```python
import jax
import jax.numpy as jnp
from jax import lax
from jax.experimental import pallas as pl
from jax.experimental.pallas import tpu as pltpu
from jax.sharding import PartitionSpec as P

LANES = 128
SMALL = pltpu.CompilerParams(vmem_limit_bytes=16 * 2**20)


def column(row, width):
    return jnp.broadcast_to(row, (width, row.shape[1])).T


def edges_kernel(*refs):
    hbm, edge_ref, gate_ref, kept, held_ref = refs[:13], refs[13], refs[14], refs[15:19], refs[19]
    vmem, sems = refs[20:29], refs[29]
    loads = [pltpu.make_async_copy(h, v, sems.at[n]) for n, (h, v) in enumerate(zip(hbm, vmem + kept))]
    for load in loads:
        load.start()
    pair_ref, gain_ref, shift_ref, lw_ref, lb_ref, rw_ref, rb_ref, gw_ref, gb_ref = vmem
    rows, cols, chans = pair_ref.shape
    hidden = lw_ref.shape[1] // 2
    for load in loads[:3]:
        load.wait()
    values = pair_ref[...].reshape(rows * cols, chans).astype(jnp.float32)
    center = values - jnp.mean(values, axis=1, keepdims=True)
    spread = jnp.mean(center * center, axis=1, keepdims=True)
    normed = (center * lax.rsqrt(spread + 1e-05) * gain_ref[...] + shift_ref[...]).astype(jnp.bfloat16)
    for load in loads[3:]:
        load.wait()
    for side, (w_ref, b_ref) in enumerate(((lw_ref, lb_ref), (rw_ref, rb_ref))):
        gate_bias = column(b_ref[:, :hidden], LANES)[:, :1]
        value_bias = column(b_ref[:, hidden:], LANES)[:, :1]
        turned = w_ref[...].T
        for r in range(rows):
            part = normed[r * cols : (r + 1) * cols]
            joined = lax.dot_general(
                turned, part, (((1,), (1,)), ((), ())), preferred_element_type=jnp.float32
            )
            edge = jax.nn.sigmoid(joined[:hidden] + gate_bias) * (joined[hidden:] + value_bias)
            held_ref[:, r, side * cols : (side + 1) * cols] = edge
    edge_ref[...] = held_ref[...].astype(jnp.bfloat16)
    gate_ref[...] = jax.nn.sigmoid(
        jnp.dot(normed, gw_ref[...], preferred_element_type=jnp.float32) + gb_ref[...]
    )


def update_kernel(tri_ref, gate_ref, gain_ref, shift_ref, w_ref, b_ref, out_ref, held_ref, made_ref, sems):
    hidden, subs, lanes = tri_ref.shape
    values = tri_ref[...].astype(jnp.float32)
    center = values - jnp.mean(values, axis=0, keepdims=True)
    spread = jnp.mean(center * center, axis=0, keepdims=True)
    held_ref[...] = center * lax.rsqrt(spread + 1e-05)
    gain = column(gain_ref[...], lanes)
    shift = column(shift_ref[...], lanes)
    stores = []
    for s in range(subs):
        mixed = (held_ref[:, s, :] * gain + shift).astype(jnp.bfloat16)
        projected = lax.dot_general(
            mixed, w_ref[...], (((0,), (0,)), ((), ())), preferred_element_type=jnp.float32
        )
        at = slice(s * lanes, (s + 1) * lanes)
        made_ref[at, :] = (gate_ref[at, :] * (projected + b_ref[...])).astype(jnp.bfloat16)
        stores.append(pltpu.make_async_copy(made_ref.at[at, :], out_ref.at[at, :], sems.at[s]))
        stores[-1].start()
    for store in stores:
        store.wait()


def per_device(
    pair_act,
    in_gain,
    in_shift,
    left_weight,
    left_bias,
    right_weight,
    right_bias,
    gate_weight,
    gate_bias,
    out_gain,
    out_shift,
    out_weight,
    out_bias,
):
    rows, cols, chans = pair_act.shape
    hidden = left_weight.shape[1] // 2
    spots = rows * cols
    peers = lax.axis_size("row")
    halves = lax.axis_size("col")
    length = peers * rows

    def row(v):
        return v.reshape(1, -1)

    given = (
        pair_act, row(in_gain), row(in_shift), left_weight, row(left_bias),
        right_weight, row(right_bias), gate_weight, row(gate_bias),
    )
    closing = (row(out_gain), row(out_shift), out_weight, row(out_bias))
    edges, gate, *closing = pl.pallas_call(
        edges_kernel,
        out_shape=(
            jax.ShapeDtypeStruct((hidden, rows, 2 * cols), jnp.bfloat16),
            jax.ShapeDtypeStruct((spots, chans), jnp.float32),
            *(jax.ShapeDtypeStruct(v.shape, v.dtype) for v in closing),
        ),
        in_specs=[pl.BlockSpec(memory_space=pltpu.HBM)] * (len(given) + len(closing)),
        scratch_shapes=[
            pltpu.VMEM((hidden, rows, 2 * cols), jnp.float32),
            *(pltpu.VMEM(v.shape, v.dtype) for v in given),
            pltpu.SemaphoreType.DMA((len(given) + len(closing),)),
        ],
        compiler_params=SMALL,
    )(*(pltpu.with_memory_space_constraint(v, pltpu.HBM) for v in (*given, *closing)))
    half = length // halves
    me = lax.axis_index("col").astype(jnp.uint32)
    edges, mine, other = lax.optimization_barrier((edges, me * half, (1 - me) * half))
    got = lax.all_to_all(edges, "row", split_axis=0, concat_axis=0, tiled=True)
    got = got.reshape(length, 2 * cols)
    left, right = got[:, :cols], got[:, cols:]

    def partial_sums(start):
        some = lax.dynamic_slice_in_dim(right, start, half, axis=0)
        return lax.dot_general(
            left, some, (((1,), (1,)), ((), ())), preferred_element_type=jnp.float32
        )

    away = lax.ppermute(partial_sums(other).astype(jnp.bfloat16), "col", [(0, 1), (1, 0)])
    triangle = (partial_sums(mine) + away.astype(jnp.float32)).astype(jnp.bfloat16)
    triangle = lax.all_to_all(
        triangle.reshape(peers, spots // LANES, LANES), "row", split_axis=0, concat_axis=0, tiled=True
    )
    update = pl.pallas_call(
        update_kernel,
        out_shape=jax.ShapeDtypeStruct((spots, chans), jnp.bfloat16),
        out_specs=pl.BlockSpec(memory_space=pltpu.HBM),
        scratch_shapes=[
            pltpu.VMEM((hidden, spots // LANES, LANES), jnp.float32),
            pltpu.VMEM((spots, chans), jnp.bfloat16),
            pltpu.SemaphoreType.DMA((spots // LANES,)),
        ],
        compiler_params=SMALL,
    )(triangle, gate, *closing)
    return update.reshape(rows, cols, chans)


def solution(mesh):
    in_specs = (P(("groups", "row"), "col", None),) + (P(),) * 12
    out_specs = P(("groups", "row"), "col", None)
    return jax.shard_map(
        per_device, mesh=mesh, in_specs=in_specs, out_specs=out_specs, check_vma=False
    )
```

```python
import jax
import jax.numpy as jnp
from jax import lax
from jax.experimental import pallas as pl
from jax.experimental.pallas import tpu as pltpu
from jax.sharding import PartitionSpec as P

LANES = 128
SMALL = pltpu.CompilerParams(vmem_limit_bytes=16 * 2**20)


def column(row, width):
    return jnp.broadcast_to(row, (width, row.shape[1])).T


def edges_kernel(*refs):
    hbm, edge_ref, gate_ref, kept, held_ref = refs[:13], refs[13], refs[14], refs[15:19], refs[19]
    vmem, sems = refs[20:29], refs[29]
    loads = [pltpu.make_async_copy(h, v, sems.at[n]) for n, (h, v) in enumerate(zip(hbm, vmem + kept))]
    for load in loads:
        load.start()
    pair_ref, gain_ref, shift_ref, lw_ref, lb_ref, rw_ref, rb_ref, gw_ref, gb_ref = vmem
    rows, cols, chans = pair_ref.shape
    hidden = lw_ref.shape[1] // 2
    for load in loads[:3]:
        load.wait()
    values = pair_ref[...].reshape(rows * cols, chans).astype(jnp.float32)
    center = values - jnp.mean(values, axis=1, keepdims=True)
    spread = jnp.mean(center * center, axis=1, keepdims=True)
    normed = (center * lax.rsqrt(spread + 1e-05) * gain_ref[...] + shift_ref[...]).astype(jnp.bfloat16)
    for load in loads[3:]:
        load.wait()
    for side, (w_ref, b_ref) in enumerate(((lw_ref, lb_ref), (rw_ref, rb_ref))):
        gate_bias = column(b_ref[:, :hidden], LANES)[:, :1]
        value_bias = column(b_ref[:, hidden:], LANES)[:, :1]
        turned = w_ref[...].T
        for r in range(rows):
            part = normed[r * cols : (r + 1) * cols]
            joined = lax.dot_general(
                turned, part, (((1,), (1,)), ((), ())), preferred_element_type=jnp.float32
            )
            edge = jax.nn.sigmoid(joined[:hidden] + gate_bias) * (joined[hidden:] + value_bias)
            for at in range(0, cols, LANES):
                block = (side * cols + at) // LANES
                held_ref[block, pl.ds(r, hidden, stride=rows), :] = edge[:, at : at + LANES]
    for block in range(held_ref.shape[0]):
        edge_ref[:, block * LANES : (block + 1) * LANES] = held_ref[block].astype(jnp.bfloat16)
    gate_ref[...] = jax.nn.sigmoid(
        jnp.dot(normed, gw_ref[...], preferred_element_type=jnp.float32) + gb_ref[...]
    )


def update_kernel(tri_ref, gate_ref, gain_ref, shift_ref, w_ref, b_ref, out_ref, held_ref, made_ref, sems):
    hidden, subs, lanes = tri_ref.shape
    values = tri_ref[...].astype(jnp.float32)
    center = values - jnp.mean(values, axis=0, keepdims=True)
    spread = jnp.mean(center * center, axis=0, keepdims=True)
    held_ref[...] = (center * lax.rsqrt(spread + 1e-05)).reshape(hidden * subs, lanes)
    gain = column(gain_ref[...], lanes)
    shift = column(shift_ref[...], lanes)
    stores = []
    for s in range(subs):
        mixed = (held_ref[pl.ds(s, hidden, stride=subs), :] * gain + shift).astype(jnp.bfloat16)
        projected = lax.dot_general(
            mixed, w_ref[...], (((0,), (0,)), ((), ())), preferred_element_type=jnp.float32
        )
        at = slice(s * lanes, (s + 1) * lanes)
        made_ref[at, :] = (gate_ref[at, :] * (projected + b_ref[...])).astype(jnp.bfloat16)
        stores.append(pltpu.make_async_copy(made_ref.at[at, :], out_ref.at[at, :], sems.at[s]))
        stores[-1].start()
    for store in stores:
        store.wait()


def per_device(
    pair_act,
    in_gain,
    in_shift,
    left_weight,
    left_bias,
    right_weight,
    right_bias,
    gate_weight,
    gate_bias,
    out_gain,
    out_shift,
    out_weight,
    out_bias,
):
    rows, cols, chans = pair_act.shape
    hidden = left_weight.shape[1] // 2
    spots = rows * cols
    peers = lax.axis_size("row")
    halves = lax.axis_size("col")
    length = peers * rows

    def row(v):
        return v.reshape(1, -1)

    given = (
        pair_act, row(in_gain), row(in_shift), left_weight, row(left_bias),
        right_weight, row(right_bias), gate_weight, row(gate_bias),
    )
    closing = (row(out_gain), row(out_shift), out_weight, row(out_bias))
    edges, gate, *closing = pl.pallas_call(
        edges_kernel,
        out_shape=(
            jax.ShapeDtypeStruct((hidden * rows, 2 * cols), jnp.bfloat16),
            jax.ShapeDtypeStruct((spots, chans), jnp.float32),
            *(jax.ShapeDtypeStruct(v.shape, v.dtype) for v in closing),
        ),
        in_specs=[pl.BlockSpec(memory_space=pltpu.HBM)] * (len(given) + len(closing)),
        scratch_shapes=[
            pltpu.VMEM((2 * cols // LANES, hidden * rows, LANES), jnp.float32),
            *(pltpu.VMEM(v.shape, v.dtype) for v in given),
            pltpu.SemaphoreType.DMA((len(given) + len(closing),)),
        ],
        compiler_params=SMALL,
    )(*(pltpu.with_memory_space_constraint(v, pltpu.HBM) for v in (*given, *closing)))
    edges = edges.reshape(hidden, rows, 2 * cols)
    half = length // halves
    me = lax.axis_index("col").astype(jnp.uint32)
    edges, mine, other = lax.optimization_barrier((edges, me * half, (1 - me) * half))
    got = lax.all_to_all(edges, "row", split_axis=0, concat_axis=0, tiled=True)
    got = got.reshape(length, 2 * cols)
    left, right = got[:, :cols], got[:, cols:]

    def partial_sums(start):
        some = lax.dynamic_slice_in_dim(right, start, half, axis=0)
        return lax.dot_general(
            left, some, (((1,), (1,)), ((), ())), preferred_element_type=jnp.float32
        )

    away = lax.ppermute(partial_sums(other).astype(jnp.bfloat16), "col", [(0, 1), (1, 0)])
    triangle = (partial_sums(mine) + away.astype(jnp.float32)).astype(jnp.bfloat16)
    triangle = lax.all_to_all(
        triangle.reshape(peers, spots // LANES, LANES), "row", split_axis=0, concat_axis=0, tiled=True
    )
    update = pl.pallas_call(
        update_kernel,
        out_shape=jax.ShapeDtypeStruct((spots, chans), jnp.bfloat16),
        out_specs=pl.BlockSpec(memory_space=pltpu.HBM),
        scratch_shapes=[
            pltpu.VMEM((hidden * spots // LANES, LANES), jnp.float32),
            pltpu.VMEM((spots, chans), jnp.bfloat16),
            pltpu.SemaphoreType.DMA((spots // LANES,)),
        ],
        compiler_params=SMALL,
    )(triangle, gate, *closing)
    return update.reshape(rows, cols, chans)


def solution(mesh):
    in_specs = (P(("groups", "row"), "col", None),) + (P(),) * 12
    out_specs = P(("groups", "row"), "col", None)
    return jax.shard_map(
        per_device, mesh=mesh, in_specs=in_specs, out_specs=out_specs, check_vma=False
    )
```

```python
import jax
import jax.numpy as jnp
from jax import lax
from jax.experimental import pallas as pl
from jax.experimental.pallas import tpu as pltpu
from jax.sharding import PartitionSpec as P

LANES = 128
SMALL = pltpu.CompilerParams(vmem_limit_bytes=16 * 2**20)


def columns(*rows):
    width = rows[0].shape[1]
    return jnp.concatenate((*rows, jnp.zeros((LANES - len(rows), width), jnp.float32))).T


def edges_kernel(*refs):
    hbm, edge_ref, gate_ref, kept, held_ref = refs[:13], refs[13], refs[14], refs[15:19], refs[19]
    vmem, sems = refs[20:29], refs[29]
    loads = [pltpu.make_async_copy(h, v, sems.at[n]) for n, (h, v) in enumerate(zip(hbm, vmem + kept))]
    for load in loads:
        load.start()
    pair_ref, gain_ref, shift_ref, lw_ref, lb_ref, rw_ref, rb_ref, gw_ref, gb_ref = vmem
    rows, cols, chans = pair_ref.shape
    hidden = lw_ref.shape[1] // 2
    for load in loads:
        load.wait()
    pair = pair_ref[...].reshape(rows * cols, chans)
    share = jnp.full((chans, chans), 1 / chans, jnp.bfloat16)
    center = pair.astype(jnp.float32) - jnp.dot(pair, share, preferred_element_type=jnp.float32)
    spread = jnp.mean(center * center, axis=1, keepdims=True)
    normed = (center * lax.rsqrt(spread + 1e-05) * gain_ref[...] + shift_ref[...]).astype(jnp.bfloat16)
    halves = [ref[:, n : n + hidden] for ref in (lb_ref, rb_ref) for n in (0, hidden)]
    biases = columns(*halves)
    for side, w_ref in enumerate((lw_ref, rw_ref)):
        gate_bias = biases[:, 2 * side : 2 * side + 1]
        value_bias = biases[:, 2 * side + 1 : 2 * side + 2]
        turned = w_ref[...].T
        for r in range(rows):
            part = normed[r * cols : (r + 1) * cols]
            joined = lax.dot_general(
                turned, part, (((1,), (1,)), ((), ())), preferred_element_type=jnp.float32
            )
            edge = jax.nn.sigmoid(joined[:hidden] + gate_bias) * (joined[hidden:] + value_bias)
            for at in range(0, cols, LANES):
                block = (side * cols + at) // LANES
                held_ref[block, pl.ds(r, hidden, stride=rows), :] = edge[:, at : at + LANES]
    for block in range(held_ref.shape[0]):
        edge_ref[:, block * LANES : (block + 1) * LANES] = held_ref[block].astype(jnp.bfloat16)
    gate_ref[...] = jax.nn.sigmoid(
        jnp.dot(normed, gw_ref[...], preferred_element_type=jnp.float32) + gb_ref[...]
    )


def update_kernel(tri_ref, gate_ref, gain_ref, shift_ref, w_ref, b_ref, out_ref, held_ref, made_ref, sems):
    hidden, subs, lanes = tri_ref.shape
    values = tri_ref[...].astype(jnp.float32)
    center = values - jnp.mean(values, axis=0, keepdims=True)
    spread = jnp.mean(center * center, axis=0, keepdims=True)
    held_ref[...] = (center * lax.rsqrt(spread + 1e-05)).reshape(hidden * subs, lanes)
    scale = columns(gain_ref[...], shift_ref[...])
    gain, shift = scale[:, :1], scale[:, 1:2]
    stores = []
    for s in range(subs):
        mixed = (held_ref[pl.ds(s, hidden, stride=subs), :] * gain + shift).astype(jnp.bfloat16)
        projected = lax.dot_general(
            mixed, w_ref[...], (((0,), (0,)), ((), ())), preferred_element_type=jnp.float32
        )
        at = slice(s * lanes, (s + 1) * lanes)
        made_ref[at, :] = (gate_ref[at, :] * (projected + b_ref[...])).astype(jnp.bfloat16)
        stores.append(pltpu.make_async_copy(made_ref.at[at, :], out_ref.at[at, :], sems.at[s]))
        stores[-1].start()
    for store in stores:
        store.wait()


def per_device(
    pair_act,
    in_gain,
    in_shift,
    left_weight,
    left_bias,
    right_weight,
    right_bias,
    gate_weight,
    gate_bias,
    out_gain,
    out_shift,
    out_weight,
    out_bias,
):
    rows, cols, chans = pair_act.shape
    hidden = left_weight.shape[1] // 2
    spots = rows * cols
    peers = lax.axis_size("row")
    halves = lax.axis_size("col")
    length = peers * rows

    def row(v):
        return v.reshape(1, -1)

    given = (
        pair_act, row(in_gain), row(in_shift), left_weight, row(left_bias),
        right_weight, row(right_bias), gate_weight, row(gate_bias),
    )
    closing = (row(out_gain), row(out_shift), out_weight, row(out_bias))
    edges, gate, *closing = pl.pallas_call(
        edges_kernel,
        out_shape=(
            jax.ShapeDtypeStruct((hidden * rows, 2 * cols), jnp.bfloat16),
            jax.ShapeDtypeStruct((spots, chans), jnp.float32),
            *(jax.ShapeDtypeStruct(v.shape, v.dtype) for v in closing),
        ),
        in_specs=[pl.BlockSpec(memory_space=pltpu.HBM)] * (len(given) + len(closing)),
        scratch_shapes=[
            pltpu.VMEM((2 * cols // LANES, hidden * rows, LANES), jnp.float32),
            *(pltpu.VMEM(v.shape, v.dtype) for v in given),
            pltpu.SemaphoreType.DMA((len(given) + len(closing),)),
        ],
        compiler_params=SMALL,
    )(*(pltpu.with_memory_space_constraint(v, pltpu.HBM) for v in (*given, *closing)))
    edges = edges.reshape(hidden, rows, 2 * cols)
    half = length // halves
    me = lax.axis_index("col").astype(jnp.uint32)
    edges, mine, other = lax.optimization_barrier((edges, me * half, (1 - me) * half))
    got = lax.all_to_all(edges, "row", split_axis=0, concat_axis=0, tiled=True)
    got = got.reshape(length, 2 * cols)
    left, right = got[:, :cols], got[:, cols:]

    def partial_sums(start):
        some = lax.dynamic_slice_in_dim(right, start, half, axis=0)
        return lax.dot_general(
            left, some, (((1,), (1,)), ((), ())), preferred_element_type=jnp.float32
        )

    away = lax.ppermute(partial_sums(other).astype(jnp.bfloat16), "col", [(0, 1), (1, 0)])
    triangle = (partial_sums(mine) + away.astype(jnp.float32)).astype(jnp.bfloat16)
    triangle = lax.all_to_all(
        triangle.reshape(peers, spots // LANES, LANES), "row", split_axis=0, concat_axis=0, tiled=True
    )
    update = pl.pallas_call(
        update_kernel,
        out_shape=jax.ShapeDtypeStruct((spots, chans), jnp.bfloat16),
        out_specs=pl.BlockSpec(memory_space=pltpu.HBM),
        scratch_shapes=[
            pltpu.VMEM((hidden * spots // LANES, LANES), jnp.float32),
            pltpu.VMEM((spots, chans), jnp.bfloat16),
            pltpu.SemaphoreType.DMA((spots // LANES,)),
        ],
        compiler_params=SMALL,
    )(triangle, gate, *closing)
    return update.reshape(rows, cols, chans)


def solution(mesh):
    in_specs = (P(("groups", "row"), "col", None),) + (P(),) * 12
    out_specs = P(("groups", "row"), "col", None)
    return jax.shard_map(
        per_device, mesh=mesh, in_specs=in_specs, out_specs=out_specs, check_vma=False
    )
```

```python
import jax
import jax.numpy as jnp
from jax import lax
from jax.experimental import pallas as pl
from jax.experimental.pallas import tpu as pltpu
from jax.sharding import PartitionSpec as P

LANES = 128
SMALL = pltpu.CompilerParams(vmem_limit_bytes=16 * 2**20)


def columns(*rows):
    width = rows[0].shape[1]
    return jnp.concatenate((*rows, jnp.zeros((LANES - len(rows), width), jnp.float32))).T


def edges_kernel(*refs):
    hbm, edge_ref, gate_ref, kept, held_ref = refs[:13], refs[13], refs[14], refs[15:19], refs[19]
    vmem, sems = refs[20:29], refs[29]
    loads = [pltpu.make_async_copy(h, v, sems.at[n]) for n, (h, v) in enumerate(zip(hbm, vmem + kept))]
    for load in loads:
        load.start()
    pair_ref, gain_ref, shift_ref, lw_ref, lb_ref, rw_ref, rb_ref, gw_ref, gb_ref = vmem
    rows, cols, chans = pair_ref.shape
    hidden = lw_ref.shape[1] // 2
    for load in loads:
        load.wait()
    pair = pair_ref[...].reshape(rows * cols, chans)
    share = jnp.full((chans, chans), 1 / chans, jnp.bfloat16)
    center = pair.astype(jnp.float32) - jnp.dot(pair, share, preferred_element_type=jnp.float32)
    spread = jnp.mean(center * center, axis=1, keepdims=True)
    normed = (center * lax.rsqrt(spread + 1e-05) * gain_ref[...] + shift_ref[...]).astype(jnp.bfloat16)
    halves = [ref[:, n : n + hidden] for ref in (lb_ref, rb_ref) for n in (0, hidden)]
    biases = columns(*halves)
    for side, w_ref in enumerate((lw_ref, rw_ref)):
        gate_bias = biases[:, 2 * side : 2 * side + 1]
        value_bias = biases[:, 2 * side + 1 : 2 * side + 2]
        turned = w_ref[...].T
        for r in range(rows):
            part = normed[r * cols : (r + 1) * cols]
            joined = lax.dot_general(
                turned, part, (((1,), (1,)), ((), ())), preferred_element_type=jnp.float32
            )
            edge = jax.nn.sigmoid(joined[:hidden] + gate_bias) * (joined[hidden:] + value_bias)
            for at in range(0, cols, LANES):
                block = (side * cols + at) // LANES
                held_ref[block, pl.ds(r, hidden, stride=rows), :] = edge[:, at : at + LANES]
    for block in range(held_ref.shape[0]):
        edge_ref[:, block * LANES : (block + 1) * LANES] = held_ref[block].astype(jnp.bfloat16)
    gate_ref[...] = jax.nn.sigmoid(
        jnp.dot(normed, gw_ref[...], preferred_element_type=jnp.float32) + gb_ref[...]
    )


def update_kernel(tri_ref, gate_ref, gain_ref, shift_ref, w_ref, b_ref, out_ref, held_ref, made_ref, sems):
    hidden, subs, lanes = tri_ref.shape
    values = tri_ref[...].astype(jnp.float32)
    center = values - jnp.mean(values, axis=0, keepdims=True)
    spread = jnp.mean(center * center, axis=0, keepdims=True)
    held_ref[...] = (center * lax.rsqrt(spread + 1e-05)).reshape(hidden * subs, lanes)
    scale = columns(gain_ref[...], shift_ref[...])
    gain, shift = scale[:, :1], scale[:, 1:2]
    stores = []
    for s in range(subs):
        mixed = (held_ref[pl.ds(s, hidden, stride=subs), :] * gain + shift).astype(jnp.bfloat16)
        projected = lax.dot_general(
            mixed, w_ref[...], (((0,), (0,)), ((), ())), preferred_element_type=jnp.float32
        )
        at = slice(s * lanes, (s + 1) * lanes)
        made_ref[at, :] = (gate_ref[at, :] * (projected + b_ref[...])).astype(jnp.bfloat16)
        stores.append(pltpu.make_async_copy(made_ref.at[at, :], out_ref.at[at, :], sems.at[s]))
        stores[-1].start()
    for store in stores:
        store.wait()


def per_device(
    pair_act,
    in_gain,
    in_shift,
    left_weight,
    left_bias,
    right_weight,
    right_bias,
    gate_weight,
    gate_bias,
    out_gain,
    out_shift,
    out_weight,
    out_bias,
):
    rows, cols, chans = pair_act.shape
    hidden = left_weight.shape[1] // 2
    spots = rows * cols
    peers = lax.axis_size("row")
    halves = lax.axis_size("col")
    length = peers * rows

    def row(v):
        return v.reshape(1, -1)

    given = (
        pair_act, row(in_gain), row(in_shift), left_weight, row(left_bias),
        right_weight, row(right_bias), gate_weight, row(gate_bias),
    )
    closing = (row(out_gain), row(out_shift), out_weight, row(out_bias))
    edges, gate, *closing = pl.pallas_call(
        edges_kernel,
        out_shape=(
            jax.ShapeDtypeStruct((hidden * rows, 2 * cols), jnp.bfloat16),
            jax.ShapeDtypeStruct((spots, chans), jnp.float32),
            *(jax.ShapeDtypeStruct(v.shape, v.dtype) for v in closing),
        ),
        in_specs=[pl.BlockSpec(memory_space=pltpu.HBM)] * (len(given) + len(closing)),
        scratch_shapes=[
            pltpu.VMEM((2 * cols // LANES, hidden * rows, LANES), jnp.float32),
            *(pltpu.VMEM(v.shape, v.dtype) for v in given),
            pltpu.SemaphoreType.DMA((len(given) + len(closing),)),
        ],
        compiler_params=SMALL,
    )(*(pltpu.with_memory_space_constraint(v, pltpu.HBM) for v in (*given, *closing)))
    edges = edges.reshape(hidden, rows, 2 * cols)
    half = length // halves
    me = lax.axis_index("col").astype(jnp.uint32)
    edges, mine, other = lax.optimization_barrier((edges, me * half, (1 - me) * half))
    first = peers // 4
    order = [(first + n) % peers for n in range(peers)]
    got = lax.all_to_all(
        edges, "row", split_axis=0, concat_axis=0, axis_index_groups=[order], tiled=True
    )
    got = got.reshape(length, 2 * cols)
    home = (peers - first) * rows
    left, right = got[:, :cols], jnp.concatenate((got[home:, cols:], got[:home, cols:]))

    def partial_sums(start):
        some = lax.dynamic_slice_in_dim(right, start, half, axis=0)
        return lax.dot_general(
            left, some, (((1,), (1,)), ((), ())), preferred_element_type=jnp.float32
        )

    away = lax.ppermute(partial_sums(other).astype(jnp.bfloat16), "col", [(0, 1), (1, 0)])
    triangle = (partial_sums(mine) + away.astype(jnp.float32)).astype(jnp.bfloat16)
    triangle = lax.all_to_all(
        triangle.reshape(peers, spots // LANES, LANES), "row", split_axis=0, concat_axis=0,
        axis_index_groups=[order], tiled=True,
    )
    update = pl.pallas_call(
        update_kernel,
        out_shape=jax.ShapeDtypeStruct((spots, chans), jnp.bfloat16),
        out_specs=pl.BlockSpec(memory_space=pltpu.HBM),
        scratch_shapes=[
            pltpu.VMEM((hidden * spots // LANES, LANES), jnp.float32),
            pltpu.VMEM((spots, chans), jnp.bfloat16),
            pltpu.SemaphoreType.DMA((spots // LANES,)),
        ],
        compiler_params=SMALL,
    )(triangle, gate, *closing)
    return update.reshape(rows, cols, chans)


def solution(mesh):
    in_specs = (P(("groups", "row"), "col", None),) + (P(),) * 12
    out_specs = P(("groups", "row"), "col", None)
    return jax.shard_map(
        per_device, mesh=mesh, in_specs=in_specs, out_specs=out_specs, check_vma=False
    )
```

```python
import jax
import jax.numpy as jnp
from jax import lax
from jax.experimental import pallas as pl
from jax.experimental.pallas import tpu as pltpu
from jax.sharding import PartitionSpec as P

LANES = 128
SMALL = pltpu.CompilerParams(vmem_limit_bytes=16 * 2**20)


def column(row, width):
    return jnp.broadcast_to(row, (width, row.shape[1])).T


def edges_kernel(*refs):
    hbm, edge_ref, gate_ref, kept, held_ref = refs[:13], refs[13], refs[14], refs[15:19], refs[19]
    vmem, sems = refs[20:29], refs[29]
    loads = [pltpu.make_async_copy(h, v, sems.at[n]) for n, (h, v) in enumerate(zip(hbm, vmem + kept))]
    for load in loads[: len(vmem)]:
        load.start()
    pair_ref, gain_ref, shift_ref, lw_ref, lb_ref, rw_ref, rb_ref, gw_ref, gb_ref = vmem
    rows, cols, chans = pair_ref.shape
    hidden = lw_ref.shape[1] // 2
    for load in loads[:3]:
        load.wait()
    values = pair_ref[...].reshape(rows * cols, chans).astype(jnp.float32)
    center = values - jnp.mean(values, axis=1, keepdims=True)
    spread = jnp.mean(center * center, axis=1, keepdims=True)
    normed = (center * lax.rsqrt(spread + 1e-05) * gain_ref[...] + shift_ref[...]).astype(jnp.bfloat16)
    for load in loads[3 : len(vmem)]:
        load.wait()
    for load in loads[len(vmem) :]:
        load.start()
    for side, (w_ref, b_ref) in enumerate(((lw_ref, lb_ref), (rw_ref, rb_ref))):
        gate_bias = column(b_ref[:, :hidden], LANES)[:, :1]
        value_bias = column(b_ref[:, hidden:], LANES)[:, :1]
        turned = w_ref[...].T
        for r in range(rows):
            part = normed[r * cols : (r + 1) * cols]
            joined = lax.dot_general(
                turned, part, (((1,), (1,)), ((), ())), preferred_element_type=jnp.float32
            )
            edge = jax.nn.sigmoid(joined[:hidden] + gate_bias) * (joined[hidden:] + value_bias)
            for at in range(0, cols, LANES):
                block = (side * cols + at) // LANES
                held_ref[block, pl.ds(r, hidden, stride=rows), :] = edge[:, at : at + LANES]
    for block in range(held_ref.shape[0]):
        turned = held_ref[block].reshape(hidden, rows, LANES)
        edge_ref[:, :, block * LANES : (block + 1) * LANES] = turned.astype(jnp.bfloat16)
    gate_ref[...] = jax.nn.sigmoid(
        jnp.dot(normed, gw_ref[...], preferred_element_type=jnp.float32) + gb_ref[...]
    )
    for load in loads[len(vmem) :]:
        load.wait()


def update_kernel(tri_ref, gate_ref, gain_ref, shift_ref, w_ref, b_ref, out_ref, held_ref, made_ref, sems):
    hidden, subs, lanes = tri_ref.shape
    values = tri_ref[...].astype(jnp.float32)
    center = values - jnp.mean(values, axis=0, keepdims=True)
    spread = jnp.mean(center * center, axis=0, keepdims=True)
    held_ref[...] = (center * lax.rsqrt(spread + 1e-05)).reshape(hidden * subs, lanes)
    gain = column(gain_ref[...], lanes)
    shift = column(shift_ref[...], lanes)
    stores = []
    for s in range(subs):
        mixed = (held_ref[pl.ds(s, hidden, stride=subs), :] * gain + shift).astype(jnp.bfloat16)
        projected = lax.dot_general(
            mixed, w_ref[...], (((0,), (0,)), ((), ())), preferred_element_type=jnp.float32
        )
        at = slice(s * lanes, (s + 1) * lanes)
        made_ref[at, :] = (gate_ref[at, :] * (projected + b_ref[...])).astype(jnp.bfloat16)
        stores.append(pltpu.make_async_copy(made_ref.at[at, :], out_ref.at[at, :], sems.at[s]))
        stores[-1].start()
    for store in stores:
        store.wait()


def per_device(
    pair_act,
    in_gain,
    in_shift,
    left_weight,
    left_bias,
    right_weight,
    right_bias,
    gate_weight,
    gate_bias,
    out_gain,
    out_shift,
    out_weight,
    out_bias,
):
    rows, cols, chans = pair_act.shape
    hidden = left_weight.shape[1] // 2
    spots = rows * cols
    peers = lax.axis_size("row")
    halves = lax.axis_size("col")
    length = peers * rows

    def row(v):
        return v.reshape(1, -1)

    given = (
        pair_act, row(in_gain), row(in_shift), left_weight, row(left_bias),
        right_weight, row(right_bias), gate_weight, row(gate_bias),
    )
    closing = (row(out_gain), row(out_shift), out_weight, row(out_bias))
    edges, gate, *closing = pl.pallas_call(
        edges_kernel,
        out_shape=(
            jax.ShapeDtypeStruct((hidden, rows, 2 * cols), jnp.bfloat16),
            jax.ShapeDtypeStruct((spots, chans), jnp.float32),
            *(jax.ShapeDtypeStruct(v.shape, v.dtype) for v in closing),
        ),
        in_specs=[pl.BlockSpec(memory_space=pltpu.HBM)] * (len(given) + len(closing)),
        scratch_shapes=[
            pltpu.VMEM((2 * cols // LANES, hidden * rows, LANES), jnp.float32),
            *(pltpu.VMEM(v.shape, v.dtype) for v in given),
            pltpu.SemaphoreType.DMA((len(given) + len(closing),)),
        ],
        compiler_params=SMALL,
    )(*(pltpu.with_memory_space_constraint(v, pltpu.HBM) for v in (*given, *closing)))
    half = length // halves
    me = lax.axis_index("col").astype(jnp.uint32)
    edges, mine, other = lax.optimization_barrier((edges, me * half, (1 - me) * half))
    got = lax.all_to_all(edges, "row", split_axis=0, concat_axis=0, tiled=True)
    got = got.reshape(length, 2 * cols)
    left, right = got[:, :cols], got[:, cols:]

    def partial_sums(start):
        some = lax.dynamic_slice_in_dim(right, start, half, axis=0)
        return lax.dot_general(
            left, some, (((1,), (1,)), ((), ())), preferred_element_type=jnp.float32
        )

    away = lax.ppermute(partial_sums(other).astype(jnp.bfloat16), "col", [(0, 1), (1, 0)])
    triangle = (partial_sums(mine) + away.astype(jnp.float32)).astype(jnp.bfloat16)
    triangle = lax.all_to_all(
        triangle.reshape(peers, spots // LANES, LANES), "row", split_axis=0, concat_axis=0, tiled=True
    )
    update = pl.pallas_call(
        update_kernel,
        out_shape=jax.ShapeDtypeStruct((spots, chans), jnp.bfloat16),
        out_specs=pl.BlockSpec(memory_space=pltpu.HBM),
        scratch_shapes=[
            pltpu.VMEM((hidden * spots // LANES, LANES), jnp.float32),
            pltpu.VMEM((spots, chans), jnp.bfloat16),
            pltpu.SemaphoreType.DMA((spots // LANES,)),
        ],
        compiler_params=SMALL,
    )(triangle, gate, *closing)
    return update.reshape(rows, cols, chans)


def solution(mesh):
    in_specs = (P(("groups", "row"), "col", None),) + (P(),) * 12
    out_specs = P(("groups", "row"), "col", None)
    return jax.shard_map(
        per_device, mesh=mesh, in_specs=in_specs, out_specs=out_specs, check_vma=False
    )
```

```python
import jax
import jax.numpy as jnp
from jax import lax
from jax.experimental import pallas as pl
from jax.experimental.pallas import tpu as pltpu
from jax.sharding import PartitionSpec as P

LANES = 128
SMALL = pltpu.CompilerParams(vmem_limit_bytes=16 * 2**20)


def columns(*rows):
    width = rows[0].shape[1]
    return jnp.concatenate((*rows, jnp.zeros((LANES - len(rows), width), jnp.float32))).T


def edges_kernel(*refs):
    hbm, edge_ref, gate_ref, kept, held_ref = refs[:13], refs[13], refs[14], refs[15:19], refs[19]
    vmem, sems = refs[20:29], refs[29]
    loads = [pltpu.make_async_copy(h, v, sems.at[n]) for n, (h, v) in enumerate(zip(hbm, vmem + kept))]
    for load in loads[: len(vmem)]:
        load.start()
    pair_ref, gain_ref, shift_ref, lw_ref, lb_ref, rw_ref, rb_ref, gw_ref, gb_ref = vmem
    rows, cols, chans = pair_ref.shape
    hidden = lw_ref.shape[1] // 2
    for load in loads[:3]:
        load.wait()
    pair = pair_ref[...].reshape(rows * cols, chans)
    share = jnp.full((chans, chans), 1 / chans, jnp.bfloat16)
    center = pair.astype(jnp.float32) - jnp.dot(pair, share, preferred_element_type=jnp.float32)
    spread = jnp.mean(center * center, axis=1, keepdims=True)
    normed = (center * lax.rsqrt(spread + 1e-05) * gain_ref[...] + shift_ref[...]).astype(jnp.bfloat16)
    for load in loads[3 : len(vmem)]:
        load.wait()
    for load in loads[len(vmem) :]:
        load.start()
    biases = columns(*(ref[:, n : n + hidden] for ref in (lb_ref, rb_ref) for n in (0, hidden)))
    for side, w_ref in enumerate((lw_ref, rw_ref)):
        gate_bias = biases[:, 2 * side : 2 * side + 1]
        value_bias = biases[:, 2 * side + 1 : 2 * side + 2]
        turned = w_ref[...].T
        for r in range(rows):
            part = normed[r * cols : (r + 1) * cols]
            joined = lax.dot_general(
                turned, part, (((1,), (1,)), ((), ())), preferred_element_type=jnp.float32
            )
            edge = jax.nn.sigmoid(joined[:hidden] + gate_bias) * (joined[hidden:] + value_bias)
            for at in range(0, cols, LANES):
                block = (side * cols + at) // LANES
                held_ref[block, pl.ds(r, hidden, stride=rows), :] = edge[:, at : at + LANES]
    for block in range(held_ref.shape[0]):
        turned = held_ref[block].reshape(hidden, rows, LANES)
        edge_ref[:, :, block * LANES : (block + 1) * LANES] = turned.astype(jnp.bfloat16)
    gate_ref[...] = jax.nn.sigmoid(
        jnp.dot(normed, gw_ref[...], preferred_element_type=jnp.float32) + gb_ref[...]
    )
    for load in loads[len(vmem) :]:
        load.wait()


def update_kernel(tri_ref, gate_ref, gain_ref, shift_ref, w_ref, b_ref, out_ref, held_ref, made_ref, sems):
    hidden, subs, lanes = tri_ref.shape
    values = tri_ref[...].astype(jnp.float32)
    center = values - jnp.mean(values, axis=0, keepdims=True)
    spread = jnp.mean(center * center, axis=0, keepdims=True)
    held_ref[...] = (center * lax.rsqrt(spread + 1e-05)).reshape(hidden * subs, lanes)
    scale = columns(gain_ref[...], shift_ref[...])
    gain, shift = scale[:, :1], scale[:, 1:2]
    stores = []
    for s in range(subs):
        mixed = (held_ref[pl.ds(s, hidden, stride=subs), :] * gain + shift).astype(jnp.bfloat16)
        projected = lax.dot_general(
            mixed, w_ref[...], (((0,), (0,)), ((), ())), preferred_element_type=jnp.float32
        )
        at = slice(s * lanes, (s + 1) * lanes)
        made_ref[at, :] = (gate_ref[at, :] * (projected + b_ref[...])).astype(jnp.bfloat16)
        stores.append(pltpu.make_async_copy(made_ref.at[at, :], out_ref.at[at, :], sems.at[s]))
        stores[-1].start()
    for store in stores:
        store.wait()


def per_device(
    pair_act,
    in_gain,
    in_shift,
    left_weight,
    left_bias,
    right_weight,
    right_bias,
    gate_weight,
    gate_bias,
    out_gain,
    out_shift,
    out_weight,
    out_bias,
):
    rows, cols, chans = pair_act.shape
    hidden = left_weight.shape[1] // 2
    spots = rows * cols
    peers = lax.axis_size("row")
    halves = lax.axis_size("col")
    length = peers * rows

    def row(v):
        return v.reshape(1, -1)

    given = (
        pair_act, row(in_gain), row(in_shift), left_weight, row(left_bias),
        right_weight, row(right_bias), gate_weight, row(gate_bias),
    )
    closing = (row(out_gain), row(out_shift), out_weight, row(out_bias))
    edges, gate, *closing = pl.pallas_call(
        edges_kernel,
        out_shape=(
            jax.ShapeDtypeStruct((hidden, rows, 2 * cols), jnp.bfloat16),
            jax.ShapeDtypeStruct((spots, chans), jnp.float32),
            *(jax.ShapeDtypeStruct(v.shape, v.dtype) for v in closing),
        ),
        in_specs=[pl.BlockSpec(memory_space=pltpu.HBM)] * (len(given) + len(closing)),
        scratch_shapes=[
            pltpu.VMEM((2 * cols // LANES, hidden * rows, LANES), jnp.float32),
            *(pltpu.VMEM(v.shape, v.dtype) for v in given),
            pltpu.SemaphoreType.DMA((len(given) + len(closing),)),
        ],
        compiler_params=SMALL,
    )(*(pltpu.with_memory_space_constraint(v, pltpu.HBM) for v in (*given, *closing)))
    half = length // halves
    me = lax.axis_index("col").astype(jnp.uint32)
    edges, mine, other = lax.optimization_barrier((edges, me * half, (1 - me) * half))
    got = lax.all_to_all(edges, "row", split_axis=0, concat_axis=0, tiled=True)
    got = got.reshape(length, 2 * cols)
    left, right = got[:, :cols], got[:, cols:]

    def partial_sums(start):
        some = lax.dynamic_slice_in_dim(right, start, half, axis=0)
        return lax.dot_general(
            left, some, (((1,), (1,)), ((), ())), preferred_element_type=jnp.float32
        )

    away = lax.ppermute(partial_sums(other).astype(jnp.bfloat16), "col", [(0, 1), (1, 0)])
    triangle = (partial_sums(mine) + away.astype(jnp.float32)).astype(jnp.bfloat16)
    triangle = lax.all_to_all(
        triangle.reshape(peers, spots // LANES, LANES), "row", split_axis=0, concat_axis=0, tiled=True
    )
    update = pl.pallas_call(
        update_kernel,
        out_shape=jax.ShapeDtypeStruct((spots, chans), jnp.bfloat16),
        out_specs=pl.BlockSpec(memory_space=pltpu.HBM),
        scratch_shapes=[
            pltpu.VMEM((hidden * spots // LANES, LANES), jnp.float32),
            pltpu.VMEM((spots, chans), jnp.bfloat16),
            pltpu.SemaphoreType.DMA((spots // LANES,)),
        ],
        compiler_params=SMALL,
    )(triangle, gate, *closing)
    return update.reshape(rows, cols, chans)


def solution(mesh):
    in_specs = (P(("groups", "row"), "col", None),) + (P(),) * 12
    out_specs = P(("groups", "row"), "col", None)
    return jax.shard_map(
        per_device, mesh=mesh, in_specs=in_specs, out_specs=out_specs, check_vma=False
    )
```
